32 devices in a mesh: freq: 8 (over z, y), pts: 4 (over x, core).
Axes of the slice: x: 2, y: 2, z: 4, core: 2. Of those that a mesh axis runs over, the one named last changes fastest.
Arguments:
- direct: bfloat16 [8, 512, 6144], P('freq', None, 'pts'), may hold values from -6 to 6
- onsets: int32 [8, 6144], P('freq', 'pts'), may hold values from 64 to 511
- left_bases: bfloat16 [128, 24, 24, 2, 8, 256], P('freq', 'pts'), may hold values from -0.4375 to 0.4375
- right_bases: bfloat16 [128, 24, 24, 2, 8, 256], P('freq', 'pts'), may hold values from -0.25 to 0.25
- tile_ranks: int32 [128, 24, 24], P('freq', 'pts'), may hold values from 1 to 8
Outputs:
- plus_field: float32 [8, 512, 6144], P('freq', None, 'pts')
- minus_field: float32 [8, 512, 6144], P('freq', None, 'pts')
The draws below stay inside these ranges and needn't reach their ends.
All inputs are finite; a program needn't handle non-finite values.
Results may differ from the reference program's by a relative error of at most 0.017.
Values may be sent and summed in bfloat16 or wider, within the bound.
A program may use at most 256 MiB of HBM per device.

```python
import math
import jax
import jax.numpy as jnp
from jax import lax

N = 6144
NB = 256
K = 8
F = 128
ITERS = 3
NT = 512
NTL = 24
P_SIZE = 8
N_PTS = 4


def place_ends(drawn, own_key, least, top_value):
    longest = drawn.shape.index(max(drawn.shape))
    spots = []
    for shift in (0, 1):
        where = [jax.random.randint(jax.random.fold_in(own_key, axis), (), 0, length) for axis, length in enumerate(drawn.shape)]
        where[longest] = (where[longest] + shift) % drawn.shape[longest]
        spots.append(tuple(where))
    return drawn.at[spots[0]].set(least).at[spots[1]].set(top_value)


def block_scale(stream_key, shape, shards, smallest, top_value):
    level = 1.0
    for position, parts in shards:
        steps = jax.random.uniform(jax.random.fold_in(jax.random.fold_in(stream_key, 6), position), (parts,), jnp.float32, smallest / len(shards), top_value / len(shards))
        level = level * jnp.repeat(jnp.exp(steps), shape[position] // parts).reshape((-1,) + (1,) * (len(shape) - 1 - position))
    return level


def gaussian(rng, dims, spread, most, cuts=(), dtype=jnp.bfloat16):
    array = spread * jax.random.normal(rng, dims, jnp.float32)
    if cuts:
        array = array * block_scale(rng, dims, cuts, -0.22, 0.18)
    return jnp.clip(array, -most, most).astype(dtype)


def setup_inputs(seed: int = 0) -> dict:
    seeds = jax.random.split(jax.random.key(seed), 6)
    return {
        "direct": gaussian(seeds[0], (P_SIZE, NT, N), 1.0, 6.0, ((0, 8), (2, 4))),
        "onsets": place_ends(jax.random.randint(seeds[1], (P_SIZE, N), NT // 8, NT), jax.random.fold_in(seeds[1], 1), NT // 8, NT - 1).astype(jnp.int32),
        "left_bases": gaussian(seeds[2], (F, NTL, NTL, 2, K, NB), (N // NB * K) ** -0.5, 0.4375, ((0, 8), (1, 4))),
        "right_bases": gaussian(seeds[3], (F, NTL, NTL, 2, K, NB), (2 * NB) ** -0.5, 0.25, ((0, 8), (1, 4))),
        "tile_ranks": place_ends(jax.random.randint(seeds[4], (F, NTL, NTL), 1, K + 1), jax.random.fold_in(seeds[4], 1), 1, K).astype(jnp.int32),
    }


HIGHEST = lax.Precision.HIGHEST

def band_tables(freq_total, sample_total):
    bins = lax.broadcasted_iota(jnp.int32, (freq_total, sample_total), 0) + 1
    moments = lax.broadcasted_iota(jnp.int32, (freq_total, sample_total), 1)
    phases = 2.0 * math.pi / sample_total * (bins * moments % sample_total).astype(jnp.float32)
    scaling = 1.0 / math.sqrt(sample_total)
    cosine = jnp.cos(phases) * scaling
    sine = jnp.sin(phases) * scaling
    return (jnp.stack([cosine, -sine]), jnp.stack([2.0 * cosine, -2.0 * sine]))

def rounded(values):
    return lax.optimization_barrier(values.astype(jnp.bfloat16)).astype(jnp.float32)

def contract(spec, left_part, right_part):
    return jnp.einsum(spec, left_part.astype(jnp.float32), right_part.astype(jnp.float32), precision=HIGHEST)

def conj_apply(spec, basis_real, basis_imag, vector_real, vector_imag):
    real_part = contract(spec, basis_real, vector_real) + contract(spec, basis_imag, vector_imag)
    imag_part = contract(spec, basis_real, vector_imag) - contract(spec, basis_imag, vector_real)
    return (real_part, imag_part)

def plain_apply(spec, basis_real, basis_imag, vector_real, vector_imag):
    real_part = contract(spec, basis_real, vector_real) - contract(spec, basis_imag, vector_imag)
    imag_part = contract(spec, basis_real, vector_imag) + contract(spec, basis_imag, vector_real)
    return (real_part, imag_part)

def reference(direct, onsets, left_bases, right_bases, tile_ranks):
    forward_exact, inverse_exact = band_tables(F, NT)
    forward_table = rounded(forward_exact)
    inverse_table = rounded(inverse_exact)
    point_total = direct.shape[0]
    tile_count = N // NB
    tile_group = tile_count // N_PTS
    moments = lax.broadcasted_iota(jnp.int32, direct.shape, 1)
    window = (moments < onsets[:, None, :]).astype(jnp.float32)
    rank_index = lax.broadcasted_iota(jnp.int32, tile_ranks.shape + (K,), 3)
    rank_mask = (rank_index < tile_ranks[..., None]).astype(jnp.float32)[..., None]

    def to_band(history):
        samples = rounded(history)
        spectrum = jnp.einsum('cft,ptn->cfpn', forward_table, samples, precision=HIGHEST)
        spectrum = spectrum.reshape(2, F, point_total, tile_count, NB).astype(jnp.bfloat16)
        return jnp.moveaxis(spectrum, 1, 0)

    def to_time(spectrum):
        flat = jnp.moveaxis(spectrum, 0, 1).reshape(2, F, point_total, N).astype(jnp.float32)
        return jnp.einsum('cft,cfpn->ptn', inverse_table, flat, precision=HIGHEST) * window

    def forward_one(operands):
        spectrum, left_part, right_part, mask_part = operands
        real_part, imag_part = conj_apply('ijkb,pjb->ijkp', right_part[:, :, 0], right_part[:, :, 1], spectrum[0], spectrum[1])
        terms = (jnp.stack([real_part, imag_part]) * mask_part).astype(jnp.bfloat16)
        real_part, imag_part = plain_apply('ijkb,ijkp->pib', left_part[:, :, 0], left_part[:, :, 1], terms[0], terms[1])
        return jnp.stack([real_part, imag_part]).astype(jnp.bfloat16)

    def adjoint_one(operands):
        spectrum, left_part, right_part, mask_part = operands
        real_part, imag_part = conj_apply('ijkb,pib->ijkp', left_part[:, :, 0], left_part[:, :, 1], spectrum[0], spectrum[1])
        terms = (jnp.stack([real_part, imag_part]) * mask_part).astype(jnp.bfloat16)
        terms = terms.reshape(2, N_PTS, tile_group, tile_count, K, point_total)
        grouped = right_part.reshape(N_PTS, tile_group, tile_count, 2, K, NB)
        real_part, imag_part = plain_apply('gijkb,gijkp->gpjb', grouped[:, :, :, 0], grouped[:, :, :, 1], terms[0], terms[1])
        partial_value = jnp.stack([real_part, imag_part], axis=1).astype(jnp.bfloat16)
        partial_value = lax.optimization_barrier(partial_value).astype(jnp.float32)
        return lax.optimization_barrier(jnp.sum(partial_value, axis=0)).astype(jnp.bfloat16)
    history = direct.astype(jnp.float32)
    plus_field = history
    minus_field = jnp.zeros_like(history)
    for iteration in range(ITERS):
        spectra = lax.map(forward_one, (to_band(history), left_bases, right_bases, rank_mask))
        reflected = to_time(spectra)
        minus_field = minus_field + reflected
        spectra = lax.map(adjoint_one, (to_band(reflected), left_bases, right_bases, rank_mask))
        history = to_time(spectra)
        plus_field = plus_field + history
    return (plus_field, minus_field)
```

```python
import math

import jax
import jax.numpy as jnp
from jax import lax
from jax.sharding import PartitionSpec as P

NB = 256
K = 8
F = 128
ITERS = 3
NT = 512


def band_tables(freq_total, sample_total):
    bins = lax.broadcasted_iota(jnp.int32, (freq_total, sample_total), 0) + 1
    moments = lax.broadcasted_iota(jnp.int32, (freq_total, sample_total), 1)
    phases = 2.0 * math.pi / sample_total * (bins * moments % sample_total).astype(jnp.float32)
    scaling = 1.0 / math.sqrt(sample_total)
    cosine = jnp.cos(phases) * scaling
    sine = jnp.sin(phases) * scaling
    return (jnp.stack([cosine, -sine]), jnp.stack([2.0 * cosine, -2.0 * sine]))


def contract(spec, left_part, right_part):
    return jnp.einsum(spec, left_part, right_part, preferred_element_type=jnp.float32)


def body(direct, onsets, left_bases, right_bases, tile_ranks):
    forward_exact, inverse_exact = band_tables(F, NT)
    forward_table = forward_exact.astype(jnp.bfloat16)
    inverse_table = inverse_exact.astype(jnp.bfloat16)
    point_here = direct.shape[0]
    cells_here = direct.shape[2]
    tile_here = cells_here // NB
    freq_here = left_bases.shape[0]
    tile_count = left_bases.shape[2]
    point_total = point_here * lax.axis_size("freq")
    group_count = lax.axis_size("pts")
    moments = lax.broadcasted_iota(jnp.int32, direct.shape, 1)
    window = (moments < onsets[:, None, :]).astype(jnp.float32)
    rank_index = lax.broadcasted_iota(jnp.int32, tile_ranks.shape + (K,), 3)
    rank_mask = (rank_index < tile_ranks[..., None]).astype(jnp.bfloat16)[..., None]

    def to_band(history):
        samples = history.astype(jnp.bfloat16)
        spectrum = jnp.einsum(
            "cft,ptn->fcpn", forward_table, samples, preferred_element_type=jnp.float32
        )
        spectrum = spectrum.astype(jnp.bfloat16).reshape(F, 2, point_here, cells_here)
        return lax.all_to_all(spectrum, "freq", split_axis=0, concat_axis=2, tiled=True)

    def to_time(spectrum):
        returned = lax.all_to_all(
            spectrum.astype(jnp.bfloat16), "freq", split_axis=2, concat_axis=0, tiled=True
        )
        return (
            jnp.einsum("cft,fcpn->ptn", inverse_table, returned, preferred_element_type=jnp.float32)
            * window
        )

    stacked_left = left_bases.reshape(freq_here, tile_here, tile_count, 2 * K, NB)
    stacked_right = right_bases.reshape(freq_here, tile_here, tile_count, 2 * K, NB)
    lines = 2 * point_total

    def tiled_lines(spectrum):
        tiled = spectrum.reshape(freq_here, lines, tile_here, NB)
        return tiled.transpose(0, 2, 1, 3)

    def conj_terms(product):
        parts = product.reshape(freq_here, tile_here, tile_count, 2, K, 2, point_total)
        real_part = parts[:, :, :, 0, :, 0] + parts[:, :, :, 1, :, 1]
        imag_part = parts[:, :, :, 0, :, 1] - parts[:, :, :, 1, :, 0]
        real_part = real_part.astype(jnp.bfloat16) * rank_mask
        imag_part = imag_part.astype(jnp.bfloat16) * rank_mask
        upper = jnp.concatenate([real_part, imag_part], axis=-1)
        lower = jnp.concatenate([-imag_part, real_part], axis=-1)
        return jnp.concatenate([upper, lower], axis=3)

    def forward_apply(spectrum):
        everywhere = lax.all_gather(tiled_lines(spectrum), "pts", axis=1, tiled=True)
        terms = conj_terms(contract("fijqb,fjnb->fijqn", stacked_right, everywhere))
        result = contract("fijqb,fijqn->finb", stacked_left, terms).astype(jnp.bfloat16)
        return result.transpose(0, 2, 1, 3).reshape(freq_here, 2, point_total, cells_here)

    def adjoint_apply(spectrum):
        terms = conj_terms(contract("fijqb,finb->fijqn", stacked_left, tiled_lines(spectrum)))
        partial_value = contract("fijqb,fijqn->fjnb", stacked_right, terms)
        partial_value = partial_value.astype(jnp.bfloat16)
        arrived = lax.all_to_all(
            partial_value.reshape(freq_here, group_count, tile_here, lines, NB),
            "pts",
            split_axis=1,
            concat_axis=1,
            tiled=True,
        )
        total = jnp.sum(arrived.astype(jnp.float32), axis=1).astype(jnp.bfloat16)
        return total.transpose(0, 2, 1, 3).reshape(freq_here, 2, point_total, cells_here)

    history = direct.astype(jnp.float32)
    plus_field = history
    minus_field = jnp.zeros_like(history)
    for iteration in range(ITERS):
        reflected = to_time(forward_apply(to_band(history)))
        minus_field = minus_field + reflected
        history = to_time(adjoint_apply(to_band(reflected)))
        plus_field = plus_field + history
    return (plus_field, minus_field)


def solution(mesh):
    return jax.shard_map(
        body,
        mesh=mesh,
        in_specs=(
            P("freq", None, "pts"),
            P("freq", "pts"),
            P("freq", "pts", None, None, None, None),
            P("freq", "pts", None, None, None, None),
            P("freq", "pts", None),
        ),
        out_specs=(P("freq", None, "pts"), P("freq", None, "pts")),
        check_vma=False,
    )
```
